32 devices in a mesh: dp: 16 (over z, y, x), member: 2 (over core).
Axes of the slice: x: 2, y: 2, z: 4, core: 2. Of those that a mesh axis runs over, the one named last changes fastest.
Arguments:
- inputs: bfloat16 [24576, 393], P(('dp', 'member')), may hold values from -256 to 256
- targets: bfloat16 [24576, 377], P(('dp', 'member')), may hold values from -6 to 6
- bootstrap: int32 [2, 24576], P('member', 'dp'), may hold values from 0 to 1535
- lower_weight: bfloat16 [2, 393, 1024], P('member'), may hold values from -0.3125 to 0.3125
- lower_shift: float32 [2, 1024], P('member'), may hold values from -3 to 3
- upper_weight: bfloat16 [2, 1024, 377], P('member'), may hold values from -0.1875 to 0.1875
- upper_shift: float32 [2, 377], P('member'), may hold values from -3 to 3
- log_var: float32 [2, 377], P('member'), may hold values from -1 to 1
Outputs:
- lower_grad: float32 [2, 1024, 393], P('member', 'dp')
- bias_grad: float32 [2, 1024], P('member', 'dp')
- upper_grad: float32 [2, 1024, 377], P('member', 'dp')
- offset_grad: float32 [2, 377], P('member')
- noise_grad: float32 [2, 377], P('member')
- member_loss: float32 [2], P('member')
The draws below stay inside these ranges and needn't reach their ends.
Inputs may be any that keep to these rules, and one draw needn't show every extreme that they name: bootstrap[m, r] is an offset within the aligned block of 1536 rows that holds row r.
All inputs are finite; a program needn't handle non-finite values.
Results may differ from the reference program's by a relative error of at most 0.00076.
Values may be sent and summed in bfloat16 or wider, within the bound.
A program may use at most 64 MiB of HBM per device.

```python
import math
import jax
import jax.numpy as jnp
from jax import lax

IN = 393
OUT = 377
H = 1024
ROWS_DEV = 1536
MEMBERS = 2
ROWS = 24576
N_DP = 16


def draw_inputs(key, part):
    keys = jax.random.split(key, 4)
    position = jnp.arange(ROWS, dtype=jnp.float32) / ROWS
    rising = (1.0 + 2.0 * position)[:, None]
    column_scale = jnp.exp(jax.random.uniform(keys[1], (1, IN), jnp.float32, math.log(0.3), math.log(3.0)))
    offset = jax.random.uniform(keys[2], (1, IN), jnp.float32, -1.0, 1.0)
    row_scale = jnp.exp(jax.random.uniform(keys[0], (ROWS, 1), jnp.float32, math.log(0.5), math.log(5.0)))
    noise = jax.random.truncated_normal(keys[3], -4.0, 4.0, (ROWS, IN), jnp.float32)
    return ((noise + offset) * row_scale * rising * column_scale).astype(jnp.bfloat16)


def set_ends(values, own_key, smallest, high):
    shape = values.shape
    index_at = [jax.random.randint(jax.random.fold_in(own_key, axis), (), 0, shape[axis]) for axis in range(len(shape))]
    values = values.at[tuple(index_at)].set(smallest)
    longest = shape.index(max(shape))
    index_at[longest] = (index_at[longest] + 1) % shape[longest]
    return values.at[tuple(index_at)].set(high)


def block_levels(key, extent, cuts, low, high):
    def one(dim, parts):
        heights = jax.random.uniform(jax.random.fold_in(jax.random.fold_in(key, 6), dim), (parts,), jnp.float32, low / len(cuts), high / len(cuts))
        return jnp.repeat(jnp.exp(heights), extent[dim] // parts).reshape((-1,) + (1,) * (len(extent) - dim - 1))

    gain = one(*cuts[0])
    for cut in cuts[1:]:
        gain = gain * one(*cut)
    return gain


def scatter_about(rng, dims, spread, reach, cuts=(), kind=jnp.bfloat16):
    result = jax.random.normal(rng, dims, jnp.float32) * spread
    if len(cuts) > 0:
        result = block_levels(rng, dims, cuts, -0.22, 0.18) * result
    return jnp.clip(result, min=-reach, max=reach).astype(kind)


def setup_inputs(seed: int = 0) -> dict:
    splits = jax.random.split(jax.random.key(seed), 9)
    inputs = draw_inputs(jax.random.fold_in(splits[8], 71), 0)
    targets = scatter_about(splits[1], (ROWS, OUT), 1.0, 6.0, ((0, 32),))
    bootstrap = set_ends(jax.random.randint(splits[2], (MEMBERS, ROWS), 0, ROWS_DEV), jax.random.fold_in(splits[2], 1), 0, ROWS_DEV - 1).astype(jnp.int32)
    lower_weight = scatter_about(splits[3], (MEMBERS, IN, H), IN ** -0.5, 0.3125, ((0, 2),))
    lower_shift = scatter_about(splits[4], (MEMBERS, H), 0.5, 3.0, ((0, 2),), jnp.float32)
    upper_weight = scatter_about(splits[5], (MEMBERS, H, OUT), H ** -0.5, 0.1875, ((0, 2),))
    upper_shift = scatter_about(splits[6], (MEMBERS, OUT), 0.5, 3.0, ((0, 2),), jnp.float32)
    log_var = jnp.clip(jax.random.uniform(splits[7], (MEMBERS, OUT), jnp.float32, -1.0, 1.0) * block_levels(splits[7], (MEMBERS, OUT), ((0, 2),), -0.4, 0.0), -1.0, 1.0)
    return {"inputs": inputs, "targets": targets, "bootstrap": bootstrap, "lower_weight": lower_weight, "lower_shift": lower_shift, "upper_weight": upper_weight, "upper_shift": upper_shift, "log_var": log_var}


def member_terms(picked, goal_rows, lower_weight, lower_shift, upper_weight, upper_shift, log_var, row_count):
    pre_act = jnp.dot(picked, lower_weight, preferred_element_type=jnp.float32) + lower_shift
    hidden = jax.nn.silu(pre_act).astype(jnp.bfloat16)
    pred_mean = jnp.dot(hidden, upper_weight, preferred_element_type=jnp.float32) + upper_shift
    residual = pred_mean - goal_rows.astype(jnp.float32)
    scaled_err = residual * jnp.exp(-log_var)
    member_loss = 0.5 * jnp.sum(residual * scaled_err + log_var) / row_count
    grad_mean = scaled_err / row_count
    offset_grad = lax.optimization_barrier(jnp.sum(grad_mean, axis=0))
    noise_grad = 0.5 * lax.optimization_barrier(jnp.sum(1.0 - residual * scaled_err, axis=0)) / row_count
    grad_half = grad_mean.astype(jnp.bfloat16)
    upper_grad = lax.dot_general(hidden, grad_half, (((0,), (0,)), ((), ())), preferred_element_type=jnp.float32)
    grad_hidden = lax.dot_general(grad_half, upper_weight, (((1,), (1,)), ((), ())), preferred_element_type=jnp.float32)
    gate_sig = jax.nn.sigmoid(pre_act)
    grad_pre = grad_hidden * gate_sig * (1.0 + pre_act * (1.0 - gate_sig))
    bias_grad = lax.optimization_barrier(jnp.sum(grad_pre, axis=0))
    pre_half = grad_pre.astype(jnp.bfloat16)
    lower_grad = lax.dot_general(pre_half, picked, (((0,), (0,)), ((), ())), preferred_element_type=jnp.float32)
    return (lower_grad, bias_grad, upper_grad, offset_grad, noise_grad, member_loss)

def stack_all(*pieces):
    return jnp.stack(pieces)

def reference(inputs, targets, bootstrap, lower_weight, lower_shift, upper_weight, upper_shift, log_var):
    values = inputs.astype(jnp.float32)
    feature_mean = lax.optimization_barrier(jnp.sum(values, axis=0)) / ROWS
    centered = values - feature_mean
    feature_var = lax.optimization_barrier(jnp.sum(centered * centered, axis=0)) / ROWS
    feature_scale = 1.0 / jnp.sqrt(feature_var + 1e-06)
    scaled = (centered * feature_scale).astype(jnp.bfloat16)
    row_blocks = scaled.reshape(N_DP, ROWS_DEV, IN)
    goal_blocks = targets.reshape(N_DP, ROWS_DEV, OUT)
    pick_blocks = bootstrap.reshape(MEMBERS, N_DP, ROWS_DEV)
    results = []
    for member in range(MEMBERS):

        def visit_block(running, block_items, member=member):
            row_block, goal_block, pick_row = block_items
            block_terms = member_terms(row_block[pick_row], goal_block[pick_row], lower_weight[member], lower_shift[member], upper_weight[member], upper_shift[member], log_var[member], ROWS_DEV)
            return (jax.tree.map(jnp.add, running, block_terms), None)
        zero_sums = (jnp.zeros((H, IN), jnp.float32), jnp.zeros((H,), jnp.float32), jnp.zeros((H, OUT), jnp.float32), jnp.zeros((OUT,), jnp.float32), jnp.zeros((OUT,), jnp.float32), jnp.zeros((), jnp.float32))
        totals, unused = lax.scan(visit_block, zero_sums, (row_blocks, goal_blocks, pick_blocks[member]))
        results.append(totals)
    lower_grad, bias_grad, upper_grad, offset_grad, noise_grad, member_loss = jax.tree.map(stack_all, *results)
    return (lower_grad, bias_grad, upper_grad, offset_grad, noise_grad, member_loss)
```

```python
import functools

import jax
import jax.numpy as jnp
from jax import lax
from jax.experimental import pallas as pl
from jax.experimental.pallas import tpu as pltpu
from jax.sharding import PartitionSpec as P

MESH = pl.DeviceIdType.MESH
LANES = 128
VMEM_LIMIT = 60 * 1024 * 1024


def pad_lanes(width):
    return -(-width // LANES) * LANES


def merge_stats(slots, count, width, each):
    total = jnp.zeros((1, width), jnp.float32)
    for i in range(count):
        total = total + slots[i, 0:1, 0:width]
    mean = total / (count * each)
    spread = jnp.zeros((1, width), jnp.float32)
    for i in range(count):
        gap = slots[i, 0:1, 0:width] / each - mean
        spread = spread + (slots[i, 1:2, 0:width] + each * (gap * gap))
    return total, spread


def rows_kernel(
    n, m, x_ref, t_ref, rows_ref, goals_ref,
    member_slots, dp_slots, member_sems, dp_sems, rows_sems, goal_sems,
):
    d, c = lax.axis_index("dp"), lax.axis_index("member")
    count, width = x_ref.shape
    barrier = pltpu.get_barrier_semaphore()
    for o in range(1, m):
        pl.semaphore_signal(barrier, 1, device_id=(d, lax.rem(c + o, m)), device_id_type=MESH)
    for o in range(1, n):
        pl.semaphore_signal(barrier, 1, device_id=(lax.rem(d + o, n), c), device_id_type=MESH)

    member_slots[c] = jnp.zeros(member_slots.shape[1:], jnp.float32)
    dp_slots[d] = jnp.zeros(dp_slots.shape[1:], jnp.float32)
    values = x_ref[...].astype(jnp.float32)
    total = jnp.sum(values, axis=0, keepdims=True)
    gap = values - total / count
    member_slots[c, 0:1, 0:width] = total
    member_slots[c, 1:2, 0:width] = jnp.sum(gap * gap, axis=0, keepdims=True)
    pl.semaphore_wait(barrier, m - 1 + n - 1)

    def to_member(src, dst, sems, o):
        return pltpu.make_async_remote_copy(
            src_ref=src, dst_ref=dst, send_sem=sems.at[0, o], recv_sem=sems.at[1, o],
            device_id=(d, lax.rem(c + o, m)), device_id_type=MESH,
        )

    stat_copies = [
        to_member(member_slots.at[c], member_slots.at[c], member_sems, o) for o in range(1, m)
    ]
    for copy in stat_copies:
        copy.start()
    goal_copies = [to_member(t_ref, goals_ref.at[c], goal_sems, o) for o in range(1, m)]
    for copy in goal_copies:
        copy.start()
    for copy in stat_copies:
        copy.wait()
    total, spread = merge_stats(member_slots, m, width, count)
    dp_slots[d, 0:1, 0:width] = total
    dp_slots[d, 1:2, 0:width] = spread
    dp_copies = [
        pltpu.make_async_remote_copy(
            src_ref=dp_slots.at[d], dst_ref=dp_slots.at[d],
            send_sem=dp_sems.at[0, o], recv_sem=dp_sems.at[1, o],
            device_id=(lax.rem(d + o, n), c), device_id_type=MESH,
        )
        for o in range(1, n)
    ]
    for copy in dp_copies:
        copy.start()
    goals_ref[c] = t_ref[...]
    edge = width // LANES * LANES
    if rows_ref.shape[2] > width:
        rows_ref[c, :, edge:] = jnp.zeros((count, rows_ref.shape[2] - edge), rows_ref.dtype)
    for copy in dp_copies:
        copy.wait()
    total, spread = merge_stats(dp_slots, n, width, count * m)
    mean = total / (count * m * n)
    scale = 1.0 / jnp.sqrt(spread / (count * m * n) + 1e-06)
    rows_ref[c, :, 0:width] = ((x_ref[...].astype(jnp.float32) - mean) * scale).astype(jnp.bfloat16)
    row_copies = [to_member(rows_ref.at[c], rows_ref.at[c], rows_sems, o) for o in range(1, m)]
    for copy in row_copies:
        copy.start()
    for copy in goal_copies + row_copies:
        copy.wait()


def shared_rows(n, m, inputs, targets):
    count, width = inputs.shape
    goal_width = targets.shape[1]
    wide = pad_lanes(width)
    rows, goals = pl.pallas_call(
        functools.partial(rows_kernel, n, m),
        out_shape=(
            jax.ShapeDtypeStruct((m, count, wide), jnp.bfloat16),
            jax.ShapeDtypeStruct((m, count, goal_width), targets.dtype),
        ),
        in_specs=[pl.BlockSpec(memory_space=pltpu.VMEM)] * 2,
        out_specs=(pl.BlockSpec(memory_space=pltpu.VMEM),) * 2,
        scratch_shapes=[
            pltpu.VMEM((m, 8, wide), jnp.float32),
            pltpu.VMEM((n, 8, wide), jnp.float32),
            pltpu.SemaphoreType.DMA((2, m)),
            pltpu.SemaphoreType.DMA((2, n)),
            pltpu.SemaphoreType.DMA((2, m)),
            pltpu.SemaphoreType.DMA((2, m)),
        ],
        compiler_params=pltpu.CompilerParams(
            collective_id=1, has_side_effects=True, vmem_limit_bytes=VMEM_LIMIT
        ),
        name="share_rows",
    )(inputs, targets)
    return rows.reshape(m * count, wide), goals.reshape(m * count, goal_width)


def bit_orders(bits):
    forward = list(range(bits))
    swapped = [1, 0] + forward[2:] if bits > 1 else forward
    late = forward[2:] + forward[:2]
    return forward, swapped, late


def grads_kernel(n, bits, plan, l_ref, u_ref, s_ref, lo_ref, uo_ref, so_ref, small, *rest):
    groups = len(plan)
    slots = [rest[g * bits:(g + 1) * bits] for g in range(groups)]
    sems, small_sems = rest[groups * bits], rest[groups * bits + 1]
    d, c = lax.axis_index("dp"), lax.axis_index("member")
    mine = [lax.rem(d // 2 ** b, 2) for b in range(bits)]
    peer = [d + (1 - 2 * mine[b]) * 2 ** b for b in range(bits)]
    barrier = pltpu.get_barrier_semaphore()
    for o in range(1, n):
        pl.semaphore_signal(barrier, 1, device_id=(lax.rem(d + o, n), c), device_id_type=MESH)
    pl.semaphore_wait(barrier, n - 1)

    def half(ref, left, bit, side, lanes):
        where = tuple(side if b == bit else slice(None) for b in left)
        return where + (slice(None), lanes)

    def begin(g, step):
        which, start, order = plan[g]
        left = [b for b in reversed(range(bits)) if b not in order[:step]]
        bit = order[step]
        if step == 0:
            ref, lanes = (l_ref, u_ref)[which], pl.ds(start, LANES)
        else:
            ref, lanes = slots[g][step - 1], slice(None)
        copy = pltpu.make_async_remote_copy(
            src_ref=ref.at[half(ref, left, bit, 1 - mine[bit], lanes)],
            dst_ref=slots[g][step],
            send_sem=sems.at[0, g, step], recv_sem=sems.at[1, g, step],
            device_id=(peer[bit], c), device_id_type=MESH,
        )
        copy.start()
        return copy, ref, half(ref, left, bit, mine[bit], lanes)

    flying = [begin(g, 0) for g in range(groups)]
    small[d] = s_ref[...]
    small_copies = [
        pltpu.make_async_remote_copy(
            src_ref=s_ref, dst_ref=small.at[d],
            send_sem=small_sems.at[0, o], recv_sem=small_sems.at[1, o],
            device_id=(lax.rem(d + o, n), c), device_id_type=MESH,
        )
        for o in range(1, n)
    ]
    for copy in small_copies:
        copy.start()
    sent = []
    for step in range(bits):
        for g in range(groups):
            copy, ref, own = flying[g]
            copy.wait_recv()
            sent.append(copy)
            landed = slots[g][step]
            summed = landed[...] + ref[own]
            if step < bits - 1:
                landed[...] = summed
                flying[g] = begin(g, step + 1)
            else:
                which, start, order = plan[g]
                (lo_ref, uo_ref)[which][:, start:start + LANES] = summed
    for copy in sent:
        copy.wait_send()
    for copy in small_copies:
        copy.wait()
    total = small[0]
    for i in range(1, n):
        total = total + small[i]
    so_ref[...] = total


def reduce_grads(n, lower, upper, small):
    bits = n.bit_length() - 1
    assert n == 2 ** bits
    share = lower.shape[0] // n
    parts = [(0, t) for t in range(0, lower.shape[1], LANES)]
    parts += [(1, t) for t in range(0, upper.shape[1], LANES)]
    forward, swapped, late = bit_orders(bits)
    pattern = [forward, swapped, late, forward, swapped, forward, swapped]
    plan = [part + (tuple(pattern[i % len(pattern)]),) for i, part in enumerate(parts)]
    tree = (2,) * bits
    slots = []
    for _ in plan:
        for step in range(bits):
            slots.append(pltpu.VMEM((2,) * (bits - 1 - step) + (share, LANES), jnp.float32))
    return pl.pallas_call(
        functools.partial(grads_kernel, n, bits, plan),
        out_shape=(
            jax.ShapeDtypeStruct((share, lower.shape[1]), jnp.float32),
            jax.ShapeDtypeStruct((share, upper.shape[1]), jnp.float32),
            jax.ShapeDtypeStruct(small.shape, jnp.float32),
        ),
        in_specs=[pl.BlockSpec(memory_space=pltpu.VMEM)] * 3,
        out_specs=(pl.BlockSpec(memory_space=pltpu.VMEM),) * 3,
        scratch_shapes=[pltpu.VMEM((n,) + small.shape, jnp.float32)]
        + slots
        + [
            pltpu.SemaphoreType.DMA((2, len(plan), bits)),
            pltpu.SemaphoreType.DMA((2, n)),
        ],
        compiler_params=pltpu.CompilerParams(
            collective_id=2, has_side_effects=True, vmem_limit_bytes=VMEM_LIMIT
        ),
        name="reduce_grads",
    )(
        lower.reshape(tree + (share, lower.shape[1])),
        upper.reshape(tree + (share, upper.shape[1])),
        small,
    )


def outer_rows(left, right):
    return lax.dot_general(
        left, right, (((0,), (0,)), ((), ())), preferred_element_type=jnp.float32
    )


def per_device(
    inputs, targets, bootstrap, lower_weight, lower_shift, upper_weight, upper_shift, log_var
):
    n, m = lax.axis_size("dp"), lax.axis_size("member")
    width, out = inputs.shape[1], targets.shape[1]
    wide, out_wide = pad_lanes(width + 1), pad_lanes(out)
    row_block, goal_block = shared_rows(n, m, inputs, targets)
    row_count = goal_block.shape[0]
    spot = lax.broadcasted_iota(jnp.int32, (row_count, row_count), 1)
    choose = (bootstrap[0][:, None] == spot).astype(jnp.bfloat16)
    picked = jnp.dot(choose, row_block, preferred_element_type=jnp.float32).astype(jnp.bfloat16)
    goal_rows = jnp.dot(choose, goal_block, preferred_element_type=jnp.float32)
    lower_weight, upper_weight = lower_weight[0], upper_weight[0]
    weight_wide = jnp.pad(lower_weight, ((0, picked.shape[1] - width), (0, 0)))
    pre_act = jnp.dot(picked, weight_wide, preferred_element_type=jnp.float32) + lower_shift[0]
    gate_sig = jax.nn.sigmoid(pre_act)
    hidden = (pre_act * gate_sig).astype(jnp.bfloat16)
    pred_mean = jnp.dot(hidden, upper_weight, preferred_element_type=jnp.float32) + upper_shift[0]
    residual = pred_mean - goal_rows
    scaled_err = residual * jnp.exp(-log_var[0])
    product = residual * scaled_err
    product_sum = jnp.sum(product, axis=0)
    member_loss = 0.5 * (jnp.sum(product_sum) + row_count * jnp.sum(log_var[0])) / row_count
    grad_mean = scaled_err / row_count
    offset_grad = jnp.sum(grad_mean, axis=0)
    noise_grad = 0.5 * jnp.sum(1.0 - product, axis=0) / row_count
    grad_half = grad_mean.astype(jnp.bfloat16)
    grad_hidden = lax.dot_general(
        grad_half, upper_weight, (((1,), (1,)), ((), ())), preferred_element_type=jnp.float32
    )
    grad_pre = grad_hidden * gate_sig * (1.0 + pre_act * (1.0 - gate_sig))
    bias = jnp.sum(grad_pre, axis=0)
    pre_half = grad_pre.astype(jnp.bfloat16)
    upper = outer_rows(hidden, jnp.pad(grad_half, ((0, 0), (0, out_wide - out))))
    lower = outer_rows(pre_half, picked)
    column = lax.broadcasted_iota(jnp.int32, lower.shape, 1)
    lower = jnp.where(column == width, bias[:, None], lower)
    small = jnp.pad(
        jnp.stack([offset_grad, noise_grad, jnp.full((out,), member_loss)]),
        ((0, 5), (0, out_wide - out)),
    )
    lower, upper, small = reduce_grads(n, lower, upper, small)
    return (
        lower[None, :, :width],
        lower[None, :, width],
        upper[None, :, :out],
        small[0:1, :out],
        small[1:2, :out],
        small[2, 0:1],
    )


def solution(mesh):
    return jax.shard_map(
        per_device,
        mesh=mesh,
        in_specs=(
            P(("dp", "member"), None),
            P(("dp", "member"), None),
            P("member", "dp"),
            P("member", None, None),
            P("member", None),
            P("member", None, None),
            P("member", None),
            P("member", None),
        ),
        out_specs=(
            P("member", "dp", None),
            P("member", "dp"),
            P("member", "dp", None),
            P("member", None),
            P("member", None),
            P("member"),
        ),
        check_vma=False,
    )
```

```python
import functools

import jax
import jax.numpy as jnp
from jax import lax
from jax.experimental import pallas as pl
from jax.experimental.pallas import tpu as pltpu
from jax.sharding import PartitionSpec as P

MESH = pl.DeviceIdType.MESH
LANES = 128
VMEM_LIMIT = 60 * 1024 * 1024


def pad_lanes(width):
    return -(-width // LANES) * LANES


def merge_stats(slots, count, width, each):
    total = jnp.zeros((1, width), jnp.float32)
    for i in range(count):
        total = total + slots[i, 0:1, 0:width]
    mean = total / (count * each)
    spread = jnp.zeros((1, width), jnp.float32)
    for i in range(count):
        gap = slots[i, 0:1, 0:width] / each - mean
        spread = spread + (slots[i, 1:2, 0:width] + each * (gap * gap))
    return total, spread


def rows_kernel(
    n, m, x_ref, t_ref, rows_ref, goals_ref,
    held, member_slots, dp_slots, member_sems, dp_sems, rows_sems, goal_sems,
):
    d, c = lax.axis_index("dp"), lax.axis_index("member")
    count, width = x_ref.shape
    barrier = pltpu.get_barrier_semaphore()
    for o in range(1, m):
        pl.semaphore_signal(barrier, 1, device_id=(d, lax.rem(c + o, m)), device_id_type=MESH)
    for o in range(1, n):
        pl.semaphore_signal(barrier, 1, device_id=(lax.rem(d + o, n), c), device_id_type=MESH)

    member_slots[c] = jnp.zeros(member_slots.shape[1:], jnp.float32)
    dp_slots[d] = jnp.zeros(dp_slots.shape[1:], jnp.float32)
    values = x_ref[...].astype(jnp.float32)
    total = jnp.sum(values, axis=0, keepdims=True)
    gap = values - total / count
    member_slots[c, 0:1, 0:width] = total
    member_slots[c, 1:2, 0:width] = jnp.sum(gap * gap, axis=0, keepdims=True)
    pl.semaphore_wait(barrier, m - 1 + n - 1)

    def to_member(src, dst, sems, o):
        return pltpu.make_async_remote_copy(
            src_ref=src, dst_ref=dst, send_sem=sems.at[0, o], recv_sem=sems.at[1, o],
            device_id=(d, lax.rem(c + o, m)), device_id_type=MESH,
        )

    stat_copies = [
        to_member(member_slots.at[c], member_slots.at[c], member_sems, o) for o in range(1, m)
    ]
    for copy in stat_copies:
        copy.start()
    row_copies = [to_member(x_ref, held.at[c], rows_sems, o) for o in range(1, m)]
    for copy in row_copies:
        copy.start()
    goal_copies = [to_member(t_ref, goals_ref.at[c], goal_sems, o) for o in range(1, m)]
    for copy in goal_copies:
        copy.start()
    for copy in stat_copies:
        copy.wait()
    total, spread = merge_stats(member_slots, m, width, count)
    dp_slots[d, 0:1, 0:width] = total
    dp_slots[d, 1:2, 0:width] = spread
    dp_copies = [
        pltpu.make_async_remote_copy(
            src_ref=dp_slots.at[d], dst_ref=dp_slots.at[d],
            send_sem=dp_sems.at[0, o], recv_sem=dp_sems.at[1, o],
            device_id=(lax.rem(d + o, n), c), device_id_type=MESH,
        )
        for o in range(1, n)
    ]
    for copy in dp_copies:
        copy.start()
    goals_ref[c] = t_ref[...]
    held[c] = x_ref[...]
    edge = width // LANES * LANES
    if rows_ref.shape[2] > width:
        rows_ref[:, :, edge:] = jnp.zeros((m, count, rows_ref.shape[2] - edge), rows_ref.dtype)
    for copy in row_copies:
        copy.wait()
    for copy in dp_copies:
        copy.wait()
    total, spread = merge_stats(dp_slots, n, width, count * m)
    mean = total / (count * m * n)
    scale = 1.0 / jnp.sqrt(spread / (count * m * n) + 1e-06)
    for i in range(m):
        values = held[i].astype(jnp.float32)
        rows_ref[i, :, 0:width] = ((values - mean) * scale).astype(jnp.bfloat16)
    for copy in goal_copies:
        copy.wait()


def shared_rows(n, m, inputs, targets):
    count, width = inputs.shape
    goal_width = targets.shape[1]
    wide = pad_lanes(width + 1)
    rows, goals = pl.pallas_call(
        functools.partial(rows_kernel, n, m),
        out_shape=(
            jax.ShapeDtypeStruct((m, count, wide), jnp.bfloat16),
            jax.ShapeDtypeStruct((m, count, goal_width), targets.dtype),
        ),
        in_specs=[pl.BlockSpec(memory_space=pltpu.VMEM)] * 2,
        out_specs=(pl.BlockSpec(memory_space=pltpu.VMEM),) * 2,
        scratch_shapes=[
            pltpu.VMEM((m, count, width), inputs.dtype),
            pltpu.VMEM((m, 8, wide), jnp.float32),
            pltpu.VMEM((n, 8, wide), jnp.float32),
            pltpu.SemaphoreType.DMA((2, m)),
            pltpu.SemaphoreType.DMA((2, n)),
            pltpu.SemaphoreType.DMA((2, m)),
            pltpu.SemaphoreType.DMA((2, m)),
        ],
        compiler_params=pltpu.CompilerParams(
            collective_id=1, has_side_effects=True, vmem_limit_bytes=VMEM_LIMIT
        ),
        name="share_rows",
    )(inputs, targets)
    return rows.reshape(m * count, wide), goals.reshape(m * count, goal_width)


def bit_orders(bits):
    forward = list(range(bits))
    swapped = [1, 0] + forward[2:] if bits > 1 else forward
    late = forward[2:] + forward[:2]
    return forward, swapped, late


def grads_kernel(n, bits, plan, l_ref, u_ref, s_ref, lo_ref, uo_ref, so_ref, small, *rest):
    groups = len(plan)
    slots = [rest[g * bits:(g + 1) * bits] for g in range(groups)]
    sems, small_sems = rest[groups * bits], rest[groups * bits + 1]
    d, c = lax.axis_index("dp"), lax.axis_index("member")
    mine = [lax.rem(d // 2 ** b, 2) for b in range(bits)]
    peer = [d + (1 - 2 * mine[b]) * 2 ** b for b in range(bits)]
    barrier = pltpu.get_barrier_semaphore()
    for o in range(1, n):
        pl.semaphore_signal(barrier, 1, device_id=(lax.rem(d + o, n), c), device_id_type=MESH)
    pl.semaphore_wait(barrier, n - 1)

    def half(ref, left, bit, side, lanes):
        where = tuple(side if b == bit else slice(None) for b in left)
        return where + (slice(None), lanes)

    def begin(g, step):
        which, start, order = plan[g]
        left = [b for b in reversed(range(bits)) if b not in order[:step]]
        bit = order[step]
        if step == 0:
            ref, lanes = (l_ref, u_ref)[which], pl.ds(start, LANES)
        else:
            ref, lanes = slots[g][step - 1], slice(None)
        copy = pltpu.make_async_remote_copy(
            src_ref=ref.at[half(ref, left, bit, 1 - mine[bit], lanes)],
            dst_ref=slots[g][step],
            send_sem=sems.at[0, g, step], recv_sem=sems.at[1, g, step],
            device_id=(peer[bit], c), device_id_type=MESH,
        )
        copy.start()
        return copy, ref, half(ref, left, bit, mine[bit], lanes)

    flying = [begin(g, 0) for g in range(groups)]
    small[d] = s_ref[...]
    small_copies = [
        pltpu.make_async_remote_copy(
            src_ref=s_ref, dst_ref=small.at[d],
            send_sem=small_sems.at[0, o], recv_sem=small_sems.at[1, o],
            device_id=(lax.rem(d + o, n), c), device_id_type=MESH,
        )
        for o in range(1, n)
    ]
    for copy in small_copies:
        copy.start()
    sent = []
    for step in range(bits):
        for g in range(groups):
            copy, ref, own = flying[g]
            copy.wait_recv()
            sent.append(copy)
            landed = slots[g][step]
            summed = landed[...] + ref[own]
            if step < bits - 1:
                landed[...] = summed
                flying[g] = begin(g, step + 1)
            else:
                which, start, order = plan[g]
                (lo_ref, uo_ref)[which][:, start:start + LANES] = summed
    for copy in sent:
        copy.wait_send()
    for copy in small_copies:
        copy.wait()
    total = small[0]
    for i in range(1, n):
        total = total + small[i]
    so_ref[...] = total


def reduce_grads(n, lower, upper, small):
    bits = n.bit_length() - 1
    assert n == 2 ** bits
    share = lower.shape[0] // n
    parts = [(0, t) for t in range(0, lower.shape[1], LANES)]
    parts += [(1, t) for t in range(0, upper.shape[1], LANES)]
    forward, swapped, late = bit_orders(bits)
    pattern = [forward, swapped, late, forward, swapped, forward, swapped]
    plan = [part + (tuple(pattern[i % len(pattern)]),) for i, part in enumerate(parts)]
    tree = (2,) * bits
    slots = []
    for _ in plan:
        for step in range(bits):
            slots.append(pltpu.VMEM((2,) * (bits - 1 - step) + (share, LANES), jnp.float32))
    return pl.pallas_call(
        functools.partial(grads_kernel, n, bits, plan),
        out_shape=(
            jax.ShapeDtypeStruct((share, lower.shape[1]), jnp.float32),
            jax.ShapeDtypeStruct((share, upper.shape[1]), jnp.float32),
            jax.ShapeDtypeStruct(small.shape, jnp.float32),
        ),
        in_specs=[pl.BlockSpec(memory_space=pltpu.VMEM)] * 3,
        out_specs=(pl.BlockSpec(memory_space=pltpu.VMEM),) * 3,
        scratch_shapes=[pltpu.VMEM((n,) + small.shape, jnp.float32)]
        + slots
        + [
            pltpu.SemaphoreType.DMA((2, len(plan), bits)),
            pltpu.SemaphoreType.DMA((2, n)),
        ],
        compiler_params=pltpu.CompilerParams(
            collective_id=2, has_side_effects=True, vmem_limit_bytes=VMEM_LIMIT
        ),
        name="reduce_grads",
    )(
        lower.reshape(tree + (share, lower.shape[1])),
        upper.reshape(tree + (share, upper.shape[1])),
        small,
    )


def outer_rows(left, right):
    return lax.dot_general(
        left, right, (((0,), (0,)), ((), ())), preferred_element_type=jnp.float32
    )


def per_device(
    inputs, targets, bootstrap, lower_weight, lower_shift, upper_weight, upper_shift, log_var
):
    n, m = lax.axis_size("dp"), lax.axis_size("member")
    width, out = inputs.shape[1], targets.shape[1]
    wide, out_wide = pad_lanes(width + 1), pad_lanes(out)
    row_block, goal_block = shared_rows(n, m, inputs, targets)
    row_count = goal_block.shape[0]
    spot = lax.broadcasted_iota(jnp.int32, (row_count, row_count), 1)
    choose = (bootstrap[0][:, None] == spot).astype(jnp.bfloat16)
    picked = jnp.dot(choose, row_block, preferred_element_type=jnp.float32).astype(jnp.bfloat16)
    goal_rows = jnp.dot(choose, goal_block, preferred_element_type=jnp.float32)
    lower_weight, upper_weight = lower_weight[0], upper_weight[0]
    weight_wide = jnp.pad(lower_weight, ((0, picked.shape[1] - width), (0, 0)))
    pre_act = jnp.dot(picked, weight_wide, preferred_element_type=jnp.float32) + lower_shift[0]
    gate_sig = jax.nn.sigmoid(pre_act)
    hidden = (pre_act * gate_sig).astype(jnp.bfloat16)
    pred_mean = jnp.dot(hidden, upper_weight, preferred_element_type=jnp.float32) + upper_shift[0]
    residual = pred_mean - goal_rows
    scaled_err = residual * jnp.exp(-log_var[0])
    product = residual * scaled_err
    product_sum = jnp.sum(product, axis=0)
    member_loss = 0.5 * (jnp.sum(product_sum) + row_count * jnp.sum(log_var[0])) / row_count
    grad_mean = scaled_err / row_count
    offset_grad = jnp.sum(grad_mean, axis=0)
    noise_grad = 0.5 * jnp.sum(1.0 - product, axis=0) / row_count
    grad_half = grad_mean.astype(jnp.bfloat16)
    grad_hidden = lax.dot_general(
        grad_half, upper_weight, (((1,), (1,)), ((), ())), preferred_element_type=jnp.float32
    )
    grad_pre = grad_hidden * gate_sig * (1.0 + pre_act * (1.0 - gate_sig))
    bias = jnp.sum(grad_pre, axis=0)
    pre_half = grad_pre.astype(jnp.bfloat16)
    upper = outer_rows(hidden, jnp.pad(grad_half, ((0, 0), (0, out_wide - out))))
    lower = outer_rows(pre_half, picked)
    column = lax.broadcasted_iota(jnp.int32, lower.shape, 1)
    lower = jnp.where(column == width, bias[:, None], lower)
    small = jnp.pad(
        jnp.stack([offset_grad, noise_grad, jnp.full((out,), member_loss)]),
        ((0, 5), (0, out_wide - out)),
    )
    lower, upper, small = reduce_grads(n, lower, upper, small)
    return (
        lower[None, :, :width],
        lower[None, :, width],
        upper[None, :, :out],
        small[0:1, :out],
        small[1:2, :out],
        small[2, 0:1],
    )


def solution(mesh):
    return jax.shard_map(
        per_device,
        mesh=mesh,
        in_specs=(
            P(("dp", "member"), None),
            P(("dp", "member"), None),
            P("member", "dp"),
            P("member", None, None),
            P("member", None),
            P("member", None, None),
            P("member", None),
            P("member", None),
        ),
        out_specs=(
            P("member", "dp", None),
            P("member", "dp"),
            P("member", "dp", None),
            P("member", None),
            P("member", None),
            P("member"),
        ),
        check_vma=False,
    )
```
